32 devices in a mesh: layer: 2 (over core), row: 4 (over y, x), col: 4 (over z).
Axes of the slice: x: 2, y: 2, z: 4, core: 2. Of those that a mesh axis runs over, the one named last changes fastest.
Arguments:
- left_matrix: bfloat16 [2048, 16384], P('row', ('layer', 'col')), may hold values from -6 to 6
- right_matrix: bfloat16 [16384, 8192], P(('layer', 'row'), 'col'), may hold values from -0.046875 to 0.046875
Outputs:
- product: bfloat16 [2048, 8192], P(('row', 'layer'), 'col')
The draws below stay inside these ranges and needn't reach their ends.
All inputs are finite; a program needn't handle non-finite values.
Results may differ from the reference program's by a relative error of at most 0.001.
Values may be sent and summed in bfloat16 or wider, within the bound.
A program may use at most 128 MiB of HBM per device.

```python
import jax
import jax.numpy as jnp

K = 16384
N = 8192
M = 2048


def block_levels(stream_key, dims, split, smallest, top_value):
    level = 1.0
    for position, blocks in split:
        heights = jax.random.uniform(jax.random.fold_in(jax.random.fold_in(stream_key, 6), position), (blocks,), jnp.float32, smallest / len(split), top_value / len(split))
        level = level * jnp.repeat(jnp.exp(heights), dims[position] // blocks).reshape((-1,) + (1,) * (len(dims) - 1 - position))
    return level


def scatter_about(rng, dims, width, bound, pieces=(), kind=jnp.bfloat16):
    array = width * jax.random.normal(rng, dims, jnp.float32)
    if pieces:
        array = array * block_levels(rng, dims, pieces, -0.22, 0.18)
    return jnp.clip(array, -bound, bound).astype(kind)


def setup_inputs(seed: int = 0) -> dict:
    keys = jax.random.split(jax.random.key(seed), 3)
    left_matrix = scatter_about(keys[0], (M, K), 1.0, 6.0, ((0, 4), (1, 8)))
    right_matrix = scatter_about(keys[1], (K, N), K ** -0.5, 0.046875, ((0, 8), (1, 4)))
    return dict(left_matrix=left_matrix, right_matrix=right_matrix)


def reference(left_matrix, right_matrix):
    exact_sum = jnp.dot(left_matrix, right_matrix, preferred_element_type=jnp.float32)
    return exact_sum.astype(jnp.bfloat16)
```

```python
import functools

import jax
import jax.numpy as jnp
from jax import lax
from jax.experimental import pallas as pl
from jax.experimental.pallas import tpu as pltpu
from jax.sharding import PartitionSpec as P

MESH = pl.DeviceIdType.MESH
CHUNK_ROWS = 16
TILE = 256
PIECES = 4


def kernel(R, NC, RB, TN, NP, a_hbm, b_hbm, o_hbm, abuf, tbuf, bbuf, cbuf, dxin, dyin, sxin, syin, obuf,
           la, ls, lr, lb, bs, br, ar, us, ws, tr, tz, tx, cd, dxr, dyr, cx, cy, sxr, syr, lo):
    l = lax.axis_index("layer")
    i = lax.axis_index("row")
    z = lax.axis_index("col")
    x = lax.rem(i, 2)
    y = lax.div(i, 2)
    xn = 2 * y + 1 - x
    yn = 2 * (1 - y) + x
    dn = 2 * (1 - y) + 1 - x
    half = NC * RB
    last = R - 1
    home = i == z
    KP = bbuf.shape[1] // NP

    def remote(src, dst, send, recv, **where):
        return pltpu.make_async_remote_copy(
            src_ref=src, dst_ref=dst, send_sem=send, recv_sem=recv,
            device_id=where, device_id_type=MESH)

    def rows(m):
        return pl.ds(m * RB if isinstance(m, int) else pl.multiple_of(m * RB, RB), RB)

    def ablock(c, m):
        return abuf.at[c, :, rows(m)]

    def own(c, act_local, act_remote):
        mine = a_hbm.at[pl.ds(pl.multiple_of(l * half + c * RB, RB), RB)]
        other = a_hbm.at[pl.ds(pl.multiple_of((1 - l) * half + c * RB, RB), RB)]

        @pl.when(home)
        def _():
            spot = abuf.at[c, l, rows(i)]
            if act_local is not None:
                act_local(pltpu.make_async_copy(mine, spot, la.at[c]))
            if act_remote is not None:
                act_remote(remote(other, spot, ls.at[c], lr.at[c], layer=1 - l))

        @pl.when(jnp.logical_not(home))
        def _():
            spot = tbuf.at[c, z, l]
            if act_local is not None:
                act_local(pltpu.make_async_copy(mine, spot, la.at[c]))
            if act_remote is not None:
                act_remote(remote(other, spot, ls.at[c], lr.at[c], layer=1 - l))

    def b_rows(p):
        return pl.ds(p * KP, KP)

    def b_load(p):
        return pltpu.make_async_copy(b_hbm.at[b_rows(p)], bbuf.at[l, b_rows(p)], lb.at[p])

    def b_swap(p):
        return remote(b_hbm.at[b_rows(p)], bbuf.at[l, b_rows(p)], bs.at[p], br.at[p], layer=1 - l)

    def cross(c, k):
        return remote(tbuf.at[c, k], ablock(c, i), tx.at[c, k], ar.at[c, i], row=k)

    def ride(c, k, step):
        return remote(tbuf.at[c, k], tbuf.at[c, k], tz.at[c, k], tr.at[c, k], col=z + step)

    def transit(c, k, act):
        act(cross(c, k))

        @pl.when((i == last) & (z < last))
        def _():
            act(ride(c, k, 1))

        @pl.when((i == 0) & (z > 0))
        def _():
            act(ride(c, k, -1))

    def passing(c, act):
        for d in range(1, R):
            for side, step in ((last, -1), (0, 1)):
                k = z + step * d

                @pl.when((i == side) & (k >= 0) & (k < R))
                def _():
                    act(c, k)

    def pass_on(c, k):
        ride(c, k, 0).wait_recv()
        transit(c, k, lambda s: s.start())

    def forward(c, m, act):
        if m < last:
            @pl.when((i <= z) & (z < last))
            def _():
                act(remote(ablock(c, m), ablock(c, m), us.at[c, m], ar.at[c, m], col=z + 1))
        if m > 0:
            @pl.when((i >= z) & (z > 0))
            def _():
                act(remote(ablock(c, m), ablock(c, m), ws.at[c, m], ar.at[c, m], col=z - 1))

    def x_first(r):
        return (r == 1) | (r == 2) | ((r == 0) & (z == 2)) | ((r == 3) & (z == 1))

    here_x = x_first(i)
    side_x = x_first(xn)
    side_y = jnp.logical_not(x_first(yn))

    def far(c, act):
        @pl.when(here_x)
        def _():
            act(remote(cbuf.at[c, rows(dn)], dxin.at[c], cd.at[c], dxr.at[c], row=xn))

        @pl.when(jnp.logical_not(here_x))
        def _():
            act(remote(cbuf.at[c, rows(dn)], dyin.at[c], cd.at[c], dyr.at[c], row=yn))

    def to_x(c):
        return remote(cbuf.at[c, rows(xn)], sxin.at[c], cx.at[c], sxr.at[c], row=xn)

    def to_y(c):
        return remote(cbuf.at[c, rows(yn)], syin.at[c], cy.at[c], syr.at[c], row=yn)

    def out(c):
        return pltpu.make_async_copy(
            obuf.at[c], o_hbm.at[pl.ds(pl.multiple_of(c * RB, RB), RB)], lo.at[c])

    @pl.loop(0, NC)
    def _(c):
        own(c, lambda s: s.start(), None)

    for p in range(NP):
        b_load(p).start()

    barrier = pltpu.get_barrier_semaphore()
    for where in ({"layer": 1 - l}, {"row": xn}, {"row": yn}, {"row": dn}):
        pl.semaphore_signal(barrier, inc=1, device_id=where, device_id_type=MESH)

    @pl.when(z > 0)
    def _():
        pl.semaphore_signal(barrier, inc=1, device_id={"col": z - 1}, device_id_type=MESH)

    @pl.when(z < last)
    def _():
        pl.semaphore_signal(barrier, inc=1, device_id={"col": z + 1}, device_id_type=MESH)

    pl.semaphore_wait(barrier, 4 + (z > 0).astype(jnp.int32) + (z < last).astype(jnp.int32))

    @pl.loop(0, NC)
    def _(c):
        own(c, None, lambda s: s.start())

    for p in range(NP):
        b_swap(p).start()

    def spread(c):
        own(c, lambda s: s.wait(), lambda s: s.wait_recv())

        @pl.when(jnp.logical_not(home))
        def _():
            transit(c, z, lambda s: s.start())

        passing(c, pass_on)
        for m in range(R):
            @pl.when(jnp.logical_not(home & (i == m)))
            def _():
                remote(ablock(c, m), ablock(c, m), us.at[c, m], ar.at[c, m], col=z).wait_recv()

            forward(c, m, lambda s: s.start())

    def multiply(c):
        @pl.loop(0, bbuf.shape[2] // TN)
        def _(n):
            part = pl.ds(pl.multiple_of(n * TN, TN), TN)
            cbuf[c, :, part] = (
                jnp.dot(abuf[c, 0], bbuf[0, :, part], preferred_element_type=jnp.float32)
                + jnp.dot(abuf[c, 1], bbuf[1, :, part], preferred_element_type=jnp.float32))
        far(c, lambda s: s.start())

    def settle(c):
        @pl.when(side_y)
        def _():
            remote(dyin.at[c], dyin.at[c], cd.at[c], dyr.at[c], row=yn).wait_recv()
            cbuf[c, rows(xn)] = cbuf[c, rows(xn)] + dyin[c]
        to_x(c).start()

        @pl.when(side_x)
        def _():
            remote(dxin.at[c], dxin.at[c], cd.at[c], dxr.at[c], row=xn).wait_recv()
            cbuf[c, rows(yn)] = cbuf[c, rows(yn)] + dxin[c]
        to_y(c).start()

    def finish(c):
        to_x(c).wait_recv()
        to_y(c).wait_recv()
        obuf[c] = (cbuf[c, rows(i)] + sxin[c] + syin[c]).astype(jnp.bfloat16)
        out(c).start()

    @pl.loop(0, NC + 2)
    def _(s):
        @pl.when(s < NC)
        def _():
            spread(s)

        @pl.when(s == 0)
        def _():
            for p in range(NP):
                b_load(p).wait()
                b_swap(p).wait_recv()

        @pl.when(s < NC)
        def _():
            multiply(s)

        @pl.when((s >= 1) & (s <= NC))
        def _():
            settle(s - 1)

        @pl.when(s >= 2)
        def _():
            finish(s - 2)

    @pl.loop(0, NC)
    def _(c):
        own(c, None, lambda s: s.wait_send())

        @pl.when(jnp.logical_not(home))
        def _():
            transit(c, z, lambda s: s.wait_send())

        passing(c, lambda c, k: transit(c, k, lambda s: s.wait_send()))
        for m in range(R):
            forward(c, m, lambda s: s.wait_send())
        far(c, lambda s: s.wait_send())
        to_x(c).wait_send()
        to_y(c).wait_send()
        out(c).wait()

    for p in range(NP):
        b_swap(p).wait_send()


def plain(left_matrix, right_matrix):
    left_rows = lax.all_gather(left_matrix, "col", axis=1, tiled=True)
    right_joined = lax.all_gather(right_matrix, "row", axis=0, tiled=True)
    summed = lax.psum_scatter(
        jnp.dot(left_rows, right_joined, preferred_element_type=jnp.float32),
        "layer",
        scatter_dimension=0,
        tiled=True,
    )
    return summed.astype(jnp.bfloat16)


def fused(R, left_matrix, right_matrix):
    rows, K = left_matrix.shape
    N = right_matrix.shape[1]
    half, RB = rows // 2, CHUNK_ROWS
    NC, NP = half // RB, PIECES
    bf16, f32 = jnp.bfloat16, jnp.float32
    dma = pltpu.SemaphoreType.DMA
    return pl.pallas_call(
        functools.partial(kernel, R, NC, RB, TILE, NP),
        out_shape=jax.ShapeDtypeStruct((half, N), bf16),
        in_specs=[pl.BlockSpec(memory_space=pl.ANY)] * 2,
        out_specs=pl.BlockSpec(memory_space=pl.ANY),
        scratch_shapes=[
            pltpu.VMEM((NC, 2, R * RB, K), bf16),
            pltpu.VMEM((NC, R, 2, RB, K), bf16),
            pltpu.VMEM((2, K, N), bf16),
            pltpu.VMEM((NC, R * RB, N), f32),
            pltpu.VMEM((NC, RB, N), f32),
            pltpu.VMEM((NC, RB, N), f32),
            pltpu.VMEM((NC, RB, N), f32),
            pltpu.VMEM((NC, RB, N), f32),
            pltpu.VMEM((NC, RB, N), bf16),
            dma((NC,)), dma((NC,)), dma((NC,)),
            dma((NP,)), dma((NP,)), dma((NP,)),
            dma((NC, R)), dma((NC, R)), dma((NC, R)),
            dma((NC, R)), dma((NC, R)), dma((NC, R)),
            dma((NC,)), dma((NC,)), dma((NC,)),
            dma((NC,)), dma((NC,)), dma((NC,)), dma((NC,)),
            dma((NC,)),
        ],
        compiler_params=pltpu.CompilerParams(
            collective_id=0, has_side_effects=True, vmem_limit_bytes=67043328),
    )(left_matrix, right_matrix)


def solution(mesh):
    shape = mesh.shape
    fits = shape["layer"] == 2 and shape["row"] == shape["col"] == 4
    local = functools.partial(fused, shape["row"]) if fits else plain
    in_specs = (P("row", ("layer", "col")), P(("layer", "row"), "col"))
    out_specs = P(("row", "layer"), "col")
    return jax.shard_map(local, mesh=mesh, in_specs=in_specs, out_specs=out_specs, check_vma=False)
```

```python
import functools

import jax
import jax.numpy as jnp
from jax import lax
from jax.experimental import pallas as pl
from jax.experimental.pallas import tpu as pltpu
from jax.sharding import PartitionSpec as P

MESH = pl.DeviceIdType.MESH
PIECE_ROWS = 16
PARTS = 4
BSTEP = 1
AHEAD = 3
RIDE = 0
RELAY = 1
DEPART = 3
HOP = 1
LAG = 1
SETTLE = 2
FINISH = 2


def kernel(R, NU, RB, TN, a_hbm, b_hbm, o_hbm, abuf, tbuf, rbuf, bbuf, cbuf, dxin, dyin, sxin, syin, obuf,
           la, ls, lr, lb, bs, br, ar, us, ws, tr, tz, tx, rr, rs, cd, dxr, dyr, cx, cy, sxr, syr, lo):
    l = lax.axis_index("layer")
    i = lax.axis_index("row")
    z = lax.axis_index("col")
    x = lax.rem(i, 2)
    y = lax.div(i, 2)
    xn = 2 * y + 1 - x
    yn = 2 * (1 - y) + x
    dn = 2 * (1 - y) + 1 - x
    half = NU // 2 * RB
    GB = 2 * RB
    NP = bbuf.shape[2] // TN
    NV = NU // 4 * NP
    last = R - 1
    home = i == z

    def remote(src, dst, send, recv, **where):
        return pltpu.make_async_remote_copy(
            src_ref=src, dst_ref=dst, send_sem=send, recv_sem=recv,
            device_id=where, device_id_type=MESH)

    def apiece(u, m):
        return abuf.at[lax.div(u, 2), pl.ds(pl.multiple_of((2 * m + lax.rem(u, 2)) * RB, RB), RB)]

    def group(m):
        return pl.ds(pl.multiple_of(m * GB, GB), GB)

    def load(w, act_local, act_remote):
        u = 4 * lax.div(w, 2) + 2 * l + lax.rem(w, 2)
        mine = a_hbm.at[pl.ds(pl.multiple_of(l * half + w * RB, RB), RB)]
        other = a_hbm.at[pl.ds(pl.multiple_of((1 - l) * half + w * RB, RB), RB)]

        def place(spot):
            if act_local is not None:
                act_local(pltpu.make_async_copy(mine, spot, la.at[w]))
            if act_remote is not None:
                act_remote(remote(other, spot, ls, lr.at[w], layer=1 - l))

        @pl.when(home)
        def _():
            place(apiece(u, i))

        @pl.when(jnp.logical_not(home))
        def _():
            place(tbuf.at[u, z])

    def loaded(u):
        w = 2 * lax.div(u, 4) + lax.rem(u, 2)
        h = lax.rem(lax.div(u, 2), 2)

        @pl.when(h == l)
        def _():
            pltpu.make_async_copy(tbuf.at[u, z], tbuf.at[u, z], la.at[w]).wait()

        @pl.when(h != l)
        def _():
            remote(tbuf.at[u, z], tbuf.at[u, z], ls, lr.at[w], layer=1 - l).wait_recv()

    def part(p):
        return pl.ds(p * TN if isinstance(p, int) else pl.multiple_of(p * TN, TN), TN)

    def b_load(p):
        return pltpu.make_async_copy(b_hbm.at[:, part(p)], bbuf.at[l, :, part(p)], lb.at[p])

    def b_swap(p):
        return remote(b_hbm.at[:, part(p)], bbuf.at[l, :, part(p)], bs, br.at[p], layer=1 - l)

    def cross(u, k, act):
        @pl.when(k == dn)
        def _():
            act(remote(tbuf.at[u, k], rbuf.at[u], tx.at[k], rr.at[u], row=xn))

        @pl.when(k != dn)
        def _():
            act(remote(tbuf.at[u, k], apiece(u, i), tx.at[k], ar.at[u, i], row=k))

    def relay(u):
        return remote(rbuf.at[u], apiece(u, xn), rs, ar.at[u, xn], row=yn)

    relaying = (z == yn) | ((xn == last) & (yn < z)) | ((xn == 0) & (yn > z))

    def onward(u, k, act):
        for side, step in ((last, 1), (0, -1)):
            @pl.when((i == side) & (z != side))
            def _():
                act(remote(tbuf.at[u, k], tbuf.at[u, k], tz.at[k], tr.at[u, k], col=z + step))

    def passing(act):
        for d in range(1, R):
            for side, step in ((last, -1), (0, 1)):
                k = z + step * d

                @pl.when((i == side) & (k >= 0) & (k < R))
                def _():
                    act(k, d)

    def forward(u, m, act):
        @pl.when((m < last) & (i <= z) & (z < last))
        def _():
            act(remote(apiece(u, m), apiece(u, m), us.at[m], ar.at[u, m], col=z + 1))

        @pl.when((m > 0) & (i >= z) & (z > 0))
        def _():
            act(remote(apiece(u, m), apiece(u, m), ws.at[m], ar.at[u, m], col=z - 1))

    def arrived(u, m):
        return remote(apiece(u, m), apiece(u, m), us.at[m], ar.at[u, m], row=xn)

    def x_first(r):
        return (r == 1) | (r == 2) | ((r == 0) & (z == 2)) | ((r == 3) & (z == 1))

    here_x = x_first(i)
    side_x = x_first(xn)
    side_y = jnp.logical_not(x_first(yn))

    def far(v, act):
        @pl.when(here_x)
        def _():
            act(remote(cbuf.at[v, group(dn)], dxin.at[v], cd, dxr.at[v], row=xn))

        @pl.when(jnp.logical_not(here_x))
        def _():
            act(remote(cbuf.at[v, group(dn)], dyin.at[v], cd, dyr.at[v], row=yn))

    def to_x(v):
        return remote(cbuf.at[v, group(xn)], sxin.at[v], cx, sxr.at[v], row=xn)

    def to_y(v):
        return remote(cbuf.at[v, group(yn)], syin.at[v], cy, syr.at[v], row=yn)

    def out(v):
        return pltpu.make_async_copy(
            obuf.at[v], o_hbm.at[group(lax.div(v, NP)), part(lax.rem(v, NP))], lo)

    @pl.loop(0, NU // 2)
    def _(w):
        load(w, lambda t: t.start(), None)

    barrier = pltpu.get_barrier_semaphore()
    for where in ({"layer": 1 - l}, {"row": xn}, {"row": yn}, {"row": dn}):
        pl.semaphore_signal(barrier, inc=1, device_id=where, device_id_type=MESH)

    @pl.when(z > 0)
    def _():
        pl.semaphore_signal(barrier, inc=1, device_id={"col": z - 1}, device_id_type=MESH)

    @pl.when(z < last)
    def _():
        pl.semaphore_signal(barrier, inc=1, device_id={"col": z + 1}, device_id_type=MESH)

    pl.semaphore_wait(barrier, 4 + (z > 0).astype(jnp.int32) + (z < last).astype(jnp.int32))

    @pl.loop(0, NU // 2)
    def _(w):
        load(w, None, lambda t: t.start())

    def launch(u):
        loaded(u)

        @pl.when(jnp.logical_not(home))
        def _():
            cross(u, z, lambda t: t.start())

    def leave(u):
        @pl.when(jnp.logical_not(home))
        def _():
            onward(u, z, lambda t: t.start())

    def pass_on(s):
        def act(k, d):
            u = s - HOP * d

            @pl.when((u >= 0) & (u < NU))
            def _():
                remote(tbuf.at[u, k], tbuf.at[u, k], tz.at[k], tr.at[u, k], row=xn).wait_recv()
                onward(u, k, lambda t: t.start())
                cross(u, k, lambda t: t.start())
        passing(act)

    def hand_on(u):
        @pl.when(relaying)
        def _():
            remote(rbuf.at[u], rbuf.at[u], rs, rr.at[u], row=xn).wait_recv()
            relay(u).start()

    def depart(u):
        @pl.when(home)
        def _():
            forward(u, i, lambda t: t.start())

    def spread(u):
        for m in (i, xn, yn, dn):
            wanted = (home & (i != m)) | ((i < z) & (m < last)) | ((i > z) & (m > 0))

            @pl.when(wanted)
            def _():
                arrived(u, m).wait_recv()
                forward(u, m, lambda t: t.start())

    def multiply(v):
        g = lax.div(v, NP)
        p = lax.rem(v, NP)

        @pl.when(p == 0)
        def _():
            @pl.when(i < z)
            def _():
                for e in range(4):
                    arrived(4 * g + e, last).wait_recv()

            @pl.when(i > z)
            def _():
                for e in range(4):
                    arrived(4 * g + e, 0).wait_recv()

        cbuf[v] = (
            jnp.dot(abuf[2 * g], bbuf[0, :, part(p)], preferred_element_type=jnp.float32)
            + jnp.dot(abuf[2 * g + 1], bbuf[1, :, part(p)], preferred_element_type=jnp.float32))
        far(v, lambda t: t.start())

    def settle(v):
        @pl.when(side_y)
        def _():
            remote(dyin.at[v], dyin.at[v], cd, dyr.at[v], row=yn).wait_recv()
            cbuf[v, group(xn)] = cbuf[v, group(xn)] + dyin[v]
        to_x(v).start()

        @pl.when(side_x)
        def _():
            remote(dxin.at[v], dxin.at[v], cd, dxr.at[v], row=xn).wait_recv()
            cbuf[v, group(yn)] = cbuf[v, group(yn)] + dxin[v]
        to_y(v).start()

    def finish(v):
        to_x(v).wait_recv()
        to_y(v).wait_recv()
        obuf[v] = (cbuf[v, group(i)] + sxin[v] + syin[v]).astype(jnp.bfloat16)
        out(v).start()

    away = HOP * jnp.abs(z - i)
    ML = 3 + LAG
    RL = RELAY + jnp.where(z == yn, -AHEAD, HOP * jnp.abs(z - yn))
    SL = HOP * last + ML + SETTLE
    FL = SL + FINISH

    @pl.loop(-AHEAD, NU + FL)
    def _(s):
        def at(lag, total, act):
            c = s - lag

            @pl.when((c >= 0) & (c < total))
            def _():
                act(c)

        for p in range(NP):
            @pl.when(s == BSTEP)
            def _():
                b_load(p).start()
                b_swap(p).start()

        at(-AHEAD, NU, launch)
        at(-RIDE, NU, leave)
        at(-DEPART, NU, depart)
        at(RL, NU, hand_on)
        pass_on(s)
        at(away, NU, spread)

        for p in range(NP):
            @pl.when(s == away + ML + p)
            def _():
                b_load(p).wait()
                b_swap(p).wait_recv()

        at(away + ML, NV, multiply)
        at(SL, NV, settle)
        at(FL, NV, finish)

    def sent(ref, sem):
        remote(ref, ref, sem, rr.at[0], row=xn).wait_send()

    def sent_on(k):
        sent(tbuf.at[:, k], tx.at[k])

        @pl.when(((i == last) & (z != last)) | ((i == 0) & (z != 0)))
        def _():
            sent(tbuf.at[:, k], tz.at[k])

    @pl.when(jnp.logical_not(home))
    def _():
        sent_on(z)

    passing(lambda k, d: sent_on(k))

    for m in range(R):
        @pl.when((m < last) & (i <= z) & (z < last))
        def _():
            sent(tbuf.at[:, m], us.at[m])

        @pl.when((m > 0) & (i >= z) & (z > 0))
        def _():
            sent(tbuf.at[:, m], ws.at[m])

    @pl.when(relaying)
    def _():
        sent(rbuf, rs)

    sent(tbuf.at[pl.ds(0, NU // 2), 0], ls)
    sent(bbuf.at[l], bs)
    sent(dxin, cd)
    sent(sxin, cx)
    sent(syin, cy)
    pltpu.make_async_copy(obuf, obuf, lo).wait()


def plain(left_matrix, right_matrix):
    left_rows = lax.all_gather(left_matrix, "col", axis=1, tiled=True)
    right_joined = lax.all_gather(right_matrix, "row", axis=0, tiled=True)
    summed = lax.psum_scatter(
        jnp.dot(left_rows, right_joined, preferred_element_type=jnp.float32),
        "layer",
        scatter_dimension=0,
        tiled=True,
    )
    return summed.astype(jnp.bfloat16)


def fused(R, left_matrix, right_matrix):
    rows, K = left_matrix.shape
    N = right_matrix.shape[1]
    half, RB, NP = rows // 2, PIECE_ROWS, PARTS
    NU, TN, GB = 2 * half // RB, N // NP, 2 * RB
    NV = NU // 4 * NP
    bf16, f32 = jnp.bfloat16, jnp.float32
    dma = pltpu.SemaphoreType.DMA
    return pl.pallas_call(
        functools.partial(kernel, R, NU, RB, TN),
        out_shape=jax.ShapeDtypeStruct((half, N), bf16),
        in_specs=[pl.BlockSpec(memory_space=pl.ANY)] * 2,
        out_specs=pl.BlockSpec(memory_space=pl.ANY),
        scratch_shapes=[
            pltpu.VMEM((NU // 2, R * GB, K), bf16),
            pltpu.VMEM((NU, R, RB, K), bf16),
            pltpu.VMEM((NU, RB, K), bf16),
            pltpu.VMEM((2, K, N), bf16),
            pltpu.VMEM((NV, R * GB, TN), f32),
            pltpu.VMEM((NV, GB, TN), f32),
            pltpu.VMEM((NV, GB, TN), f32),
            pltpu.VMEM((NV, GB, TN), f32),
            pltpu.VMEM((NV, GB, TN), f32),
            pltpu.VMEM((NV, GB, TN), bf16),
            dma((NU // 2,)), dma, dma((NU // 2,)),
            dma((NP,)), dma, dma((NP,)),
            dma((NU, R)), dma((R,)), dma((R,)),
            dma((NU, R)), dma((R,)), dma((R,)),
            dma((NU,)), dma,
            dma, dma((NV,)), dma((NV,)),
            dma, dma, dma((NV,)), dma((NV,)),
            dma,
        ],
        compiler_params=pltpu.CompilerParams(
            collective_id=0, has_side_effects=True, vmem_limit_bytes=67043328),
    )(left_matrix, right_matrix)


def solution(mesh):
    shape = mesh.shape
    fits = shape["layer"] == 2 and shape["row"] == shape["col"] == 4
    local = functools.partial(fused, shape["row"]) if fits else plain
    in_specs = (P("row", ("layer", "col")), P(("layer", "row"), "col"))
    out_specs = P(("row", "layer"), "col")
    return jax.shard_map(local, mesh=mesh, in_specs=in_specs, out_specs=out_specs, check_vma=False)
```

```python
import functools

import jax
import jax.numpy as jnp
from jax import lax
from jax.experimental import pallas as pl
from jax.experimental.pallas import tpu as pltpu
from jax.sharding import PartitionSpec as P

MESH = pl.DeviceIdType.MESH
PIECE_ROWS = 16
PARTS = 2
BSTEP = 1
AHEAD = 3
RIDE = 2
RELAY = 1
DEPART = 2
HOP = 1
LAG = 1
SETTLE = 2
FINISH = 4


def kernel(R, NU, RB, TN, a_hbm, b_hbm, o_hbm, abuf, tbuf, rbuf, bbuf, cbuf, dxin, dyin, sums, obuf,
           la, ls, lr, lb, bs, br, ar, us, ws, tr, tz, tx, rr, rs, cd, dxr, dyr, cx, cy, sr, lo):
    l = lax.axis_index("layer")
    i = lax.axis_index("row")
    z = lax.axis_index("col")
    x = lax.rem(i, 2)
    y = lax.div(i, 2)
    xn = 2 * y + 1 - x
    yn = 2 * (1 - y) + x
    dn = 2 * (1 - y) + 1 - x
    half = NU // 2 * RB
    NP = bbuf.shape[2] // TN
    NV = NU // 2 * NP
    last = R - 1
    home = i == z

    def remote(src, dst, send, recv, **where):
        return pltpu.make_async_remote_copy(
            src_ref=src, dst_ref=dst, send_sem=send, recv_sem=recv,
            device_id=where, device_id_type=MESH)

    def apiece(u, m):
        return abuf.at[u, group(m)]

    def group(m):
        return pl.ds(pl.multiple_of(m * RB, RB), RB)

    def load(w, act_local, act_remote):
        u = 2 * w + l
        mine = a_hbm.at[pl.ds(pl.multiple_of(l * half + w * RB, RB), RB)]
        other = a_hbm.at[pl.ds(pl.multiple_of((1 - l) * half + w * RB, RB), RB)]

        def place(spot):
            if act_local is not None:
                act_local(pltpu.make_async_copy(mine, spot, la.at[w]))
            if act_remote is not None:
                act_remote(remote(other, spot, ls, lr.at[w], layer=1 - l))

        @pl.when(home)
        def _():
            place(apiece(u, i))

        @pl.when(jnp.logical_not(home))
        def _():
            place(tbuf.at[u, z])

    def loaded(u):
        w = lax.div(u, 2)
        h = lax.rem(u, 2)

        @pl.when(h == l)
        def _():
            pltpu.make_async_copy(tbuf.at[u, z], tbuf.at[u, z], la.at[w]).wait()

        @pl.when(h != l)
        def _():
            remote(tbuf.at[u, z], tbuf.at[u, z], ls, lr.at[w], layer=1 - l).wait_recv()

    def part(p):
        return pl.ds(p * TN if isinstance(p, int) else pl.multiple_of(p * TN, TN), TN)

    def b_load(p):
        return pltpu.make_async_copy(b_hbm.at[:, part(p)], bbuf.at[l, :, part(p)], lb.at[p])

    def b_swap(p):
        return remote(b_hbm.at[:, part(p)], bbuf.at[l, :, part(p)], bs, br.at[p], layer=1 - l)

    def cross(u, k, act):
        @pl.when(k == dn)
        def _():
            act(remote(tbuf.at[u, k], rbuf.at[u], tx.at[k], rr.at[u], row=xn))

        @pl.when(k != dn)
        def _():
            act(remote(tbuf.at[u, k], apiece(u, i), tx.at[k], ar.at[u, i], row=k))

    def relay(u):
        return remote(rbuf.at[u], apiece(u, xn), rs, ar.at[u, xn], row=yn)

    relaying = (z == yn) | ((xn == last) & (yn < z)) | ((xn == 0) & (yn > z))

    def onward(u, k, act):
        for side, step in ((last, 1), (0, -1)):
            @pl.when((i == side) & (z != side))
            def _():
                act(remote(tbuf.at[u, k], tbuf.at[u, k], tz.at[k], tr.at[u, jnp.abs(k - z)], col=z + step))

    def passing(act):
        for d in range(1, R):
            for side, step in ((last, -1), (0, 1)):
                k = z + step * d

                @pl.when((i == side) & (k >= 0) & (k < R))
                def _():
                    act(k, d)

    def forward(u, m, act):
        @pl.when((m < last) & (i <= z) & (z < last))
        def _():
            act(remote(apiece(u, m), apiece(u, m), us.at[m], ar.at[u, m], col=z + 1))

        @pl.when((m > 0) & (i >= z) & (z > 0))
        def _():
            act(remote(apiece(u, m), apiece(u, m), ws.at[m], ar.at[u, m], col=z - 1))

    def arrived(u, m):
        return remote(apiece(u, m), apiece(u, m), us.at[m], ar.at[u, m], row=xn)

    def x_first(r):
        return (r == 1) | (r == 2) | ((r == 0) & (z == 2)) | ((r == 3) & (z == 1))

    here_x = x_first(i)
    side_x = x_first(xn)
    side_y = jnp.logical_not(x_first(yn))

    def far(v, act):
        @pl.when(here_x)
        def _():
            act(remote(cbuf.at[v, group(dn)], dxin.at[v], cd, dxr.at[v], row=xn))

        @pl.when(jnp.logical_not(here_x))
        def _():
            act(remote(cbuf.at[v, group(dn)], dyin.at[v], cd, dyr.at[v], row=yn))

    def to_x(v):
        return remote(cbuf.at[v, group(xn)], sums.at[v, 0], cx, sr.at[v], row=xn)

    def to_y(v):
        return remote(cbuf.at[v, group(yn)], sums.at[v, 1], cy, sr.at[v], row=yn)

    def out(v):
        return pltpu.make_async_copy(
            obuf.at[v], o_hbm.at[group(lax.div(v, NP)), part(lax.rem(v, NP))], lo)

    @pl.loop(0, NU // 2)
    def _(w):
        load(w, lambda t: t.start(), None)

    barrier = pltpu.get_barrier_semaphore()
    for where in ({"layer": 1 - l}, {"row": xn}, {"row": yn}, {"row": dn}):
        pl.semaphore_signal(barrier, inc=1, device_id=where, device_id_type=MESH)

    @pl.when(z > 0)
    def _():
        pl.semaphore_signal(barrier, inc=1, device_id={"col": z - 1}, device_id_type=MESH)

    @pl.when(z < last)
    def _():
        pl.semaphore_signal(barrier, inc=1, device_id={"col": z + 1}, device_id_type=MESH)

    pl.semaphore_wait(barrier, 4 + (z > 0).astype(jnp.int32) + (z < last).astype(jnp.int32))

    @pl.loop(0, NU // 2)
    def _(w):
        load(w, None, lambda t: t.start())

    def launch(u):
        loaded(u)

        @pl.when(jnp.logical_not(home))
        def _():
            cross(u, z, lambda t: t.start())

    def leave(u):
        @pl.when(jnp.logical_not(home))
        def _():
            onward(u, z, lambda t: t.start())

    def pass_on(s):
        def act(k, d):
            u = s - HOP * d + RIDE

            @pl.when((u >= 0) & (u < NU))
            def _():
                remote(tbuf.at[u, k], tbuf.at[u, k], tz.at[k], tr.at[u, d - 1], row=xn).wait_recv()
                onward(u, k, lambda t: t.start())
                cross(u, k, lambda t: t.start())
        passing(act)

    def hand_on(u):
        @pl.when(relaying)
        def _():
            remote(rbuf.at[u], rbuf.at[u], rs, rr.at[u], row=xn).wait_recv()
            relay(u).start()

    def depart(u):
        @pl.when(jnp.logical_not(home))
        def _():
            arrived(u, i).wait_recv()

        forward(u, i, lambda t: t.start())

    def spread(u):
        for m in (xn, yn, dn):
            wanted = home | ((i < z) & (m < last)) | ((i > z) & (m > 0))

            @pl.when(wanted)
            def _():
                arrived(u, m).wait_recv()
                forward(u, m, lambda t: t.start())

    def multiply(v):
        g = lax.div(v, NP)
        p = lax.rem(v, NP)

        @pl.when(p == 0)
        def _():
            @pl.when(i < z)
            def _():
                for e in range(2):
                    arrived(2 * g + e, last).wait_recv()

            @pl.when(i > z)
            def _():
                for e in range(2):
                    arrived(2 * g + e, 0).wait_recv()

        dots(v, 0)

    def dots(v, e):
        g = lax.div(v, NP)
        width = TN // 2
        columns = pl.ds(pl.multiple_of(lax.rem(v, NP) * TN + e * width, width), width)
        cbuf[v, :, e * width:(e + 1) * width] = (
            jnp.dot(abuf[2 * g], bbuf[0, :, columns], preferred_element_type=jnp.float32)
            + jnp.dot(abuf[2 * g + 1], bbuf[1, :, columns], preferred_element_type=jnp.float32))

    def partials(v):
        dots(v, 1)
        far(v, lambda t: t.start())

        @pl.when(jnp.logical_not(side_y))
        def _():
            to_x(v).start()

        @pl.when(jnp.logical_not(side_x))
        def _():
            to_y(v).start()

    def settle_x(v):
        @pl.when(side_y)
        def _():
            remote(dyin.at[v], dyin.at[v], cd, dyr.at[v], row=yn).wait_recv()
            cbuf[v, group(xn)] = cbuf[v, group(xn)] + dyin[v]
            to_x(v).start()

    def settle_y(v):
        @pl.when(side_x)
        def _():
            remote(dxin.at[v], dxin.at[v], cd, dxr.at[v], row=xn).wait_recv()
            cbuf[v, group(yn)] = cbuf[v, group(yn)] + dxin[v]
            to_y(v).start()

    def finish(v):
        remote(sums.at[v], sums.at[v], cx, sr.at[v], row=xn).wait_recv()
        obuf[v] = (cbuf[v, group(i)] + sums[v, 0] + sums[v, 1]).astype(jnp.bfloat16)
        out(v).start()

    away = HOP * jnp.abs(z - i)
    ML = 1 + LAG
    RL = RELAY + jnp.where(z == yn, -AHEAD, HOP * jnp.abs(z - yn) - RIDE)
    SL = HOP * last + ML + 1 + SETTLE
    FL = SL + FINISH

    @pl.loop(-max(AHEAD, RIDE, DEPART), NU + FL)
    def _(s):
        def at(lag, total, act):
            c = s - lag

            @pl.when((c >= 0) & (c < total))
            def _():
                act(c)

        for p in range(NP):
            @pl.when(s == BSTEP)
            def _():
                b_load(p).start()
                b_swap(p).start()

        at(-AHEAD, NU, launch)
        at(-RIDE, NU, leave)
        at(away - DEPART, NU, depart)
        at(RL, NU, hand_on)
        pass_on(s)
        at(away + ML + 1, NV, partials)
        at(away, NU, spread)

        for p in range(NP):
            @pl.when(s == away + ML + p)
            def _():
                b_load(p).wait()
                b_swap(p).wait_recv()

        at(away + ML, NV, multiply)
        at(ML + 1 + SETTLE + jnp.maximum(away, HOP * jnp.abs(z - yn)), NV, settle_x)
        at(ML + 1 + SETTLE + jnp.maximum(away, HOP * jnp.abs(z - xn)), NV, settle_y)
        at(FL, NV, finish)

    def sent(ref, sem):
        remote(ref, ref, sem, rr.at[0], row=xn).wait_send()

    def sent_on(k):
        sent(tbuf.at[:, k], tx.at[k])

        @pl.when(((i == last) & (z != last)) | ((i == 0) & (z != 0)))
        def _():
            sent(tbuf.at[:, k], tz.at[k])

    @pl.when(jnp.logical_not(home))
    def _():
        sent_on(z)

    passing(lambda k, d: sent_on(k))

    for m in range(R):
        @pl.when((m < last) & (i <= z) & (z < last))
        def _():
            sent(tbuf.at[:, m], us.at[m])

        @pl.when((m > 0) & (i >= z) & (z > 0))
        def _():
            sent(tbuf.at[:, m], ws.at[m])

    @pl.when(relaying)
    def _():
        sent(rbuf, rs)

    sent(tbuf.at[pl.ds(0, NU // 2), 0], ls)
    sent(bbuf.at[l], bs)
    sent(dxin, cd)
    sent(dxin, cx)
    sent(dxin, cy)
    pltpu.make_async_copy(obuf, obuf, lo).wait()


def plain(left_matrix, right_matrix):
    left_rows = lax.all_gather(left_matrix, "col", axis=1, tiled=True)
    right_joined = lax.all_gather(right_matrix, "row", axis=0, tiled=True)
    summed = lax.psum_scatter(
        jnp.dot(left_rows, right_joined, preferred_element_type=jnp.float32),
        "layer",
        scatter_dimension=0,
        tiled=True,
    )
    return summed.astype(jnp.bfloat16)


def fused(R, left_matrix, right_matrix):
    rows, K = left_matrix.shape
    N = right_matrix.shape[1]
    half, RB, NP = rows // 2, PIECE_ROWS, PARTS
    NU, TN, GB = 2 * half // RB, N // NP, RB
    NV = NU // 2 * NP
    bf16, f32 = jnp.bfloat16, jnp.float32
    dma = pltpu.SemaphoreType.DMA
    return pl.pallas_call(
        functools.partial(kernel, R, NU, RB, TN),
        out_shape=jax.ShapeDtypeStruct((half, N), bf16),
        in_specs=[pl.BlockSpec(memory_space=pl.ANY)] * 2,
        out_specs=pl.BlockSpec(memory_space=pl.ANY),
        scratch_shapes=[
            pltpu.VMEM((NU, R * RB, K), bf16),
            pltpu.VMEM((NU, R, RB, K), bf16),
            pltpu.VMEM((NU, RB, K), bf16),
            pltpu.VMEM((2, K, N), bf16),
            pltpu.VMEM((NV, R * GB, TN), f32),
            pltpu.VMEM((NV, GB, TN), f32),
            pltpu.VMEM((NV, GB, TN), f32),
            pltpu.VMEM((NV, 2, GB, TN), f32),
            pltpu.VMEM((NV, GB, TN), bf16),
            dma((NU // 2,)), dma, dma((NU // 2,)),
            dma((NP,)), dma, dma((NP,)),
            dma((NU, R)), dma((R,)), dma((R,)),
            dma((NU, R - 1)), dma((R,)), dma((R,)),
            dma((NU,)), dma,
            dma, dma((NV,)), dma((NV,)),
            dma, dma, dma((NV,)),
            dma,
        ],
        compiler_params=pltpu.CompilerParams(
            collective_id=0, has_side_effects=True, vmem_limit_bytes=67043328),
    )(left_matrix, right_matrix)


def solution(mesh):
    shape = mesh.shape
    fits = shape["layer"] == 2 and shape["row"] == shape["col"] == 4
    local = functools.partial(fused, shape["row"]) if fits else plain
    in_specs = (P("row", ("layer", "col")), P(("layer", "row"), "col"))
    out_specs = P(("row", "layer"), "col")
    return jax.shard_map(local, mesh=mesh, in_specs=in_specs, out_specs=out_specs, check_vma=False)
```

```python
import functools

import jax
import jax.numpy as jnp
from jax import lax
from jax.experimental import pallas as pl
from jax.experimental.pallas import tpu as pltpu
from jax.sharding import PartitionSpec as P

MESH = pl.DeviceIdType.MESH
PIECE_ROWS = 16
PARTS = 2
BSTEP = 1
AHEAD = 2
RIDE = 2
RELAY = 1
DEPART = 2
HOP = 1
LAG = 1
SETTLE = 2
FINISH = 4


def kernel(R, NU, RB, TN, a_hbm, b_hbm, o_hbm, abuf, tbuf, rbuf, bbuf, cbuf, dxin, dyin, sums, obuf,
           la, ls, lr, lb, bs, br, ar, us, ws, tr, tz, tx, rr, rs, cd, dxr, dyr, cx, cy, sr, lo):
    l = lax.axis_index("layer")
    i = lax.axis_index("row")
    z = lax.axis_index("col")
    x = lax.rem(i, 2)
    y = lax.div(i, 2)
    xn = 2 * y + 1 - x
    yn = 2 * (1 - y) + x
    dn = 2 * (1 - y) + 1 - x
    half = NU // 2 * RB
    NP = bbuf.shape[2] // TN
    NV = NU // 2 * NP
    last = R - 1
    home = i == z

    def remote(src, dst, send, recv, **where):
        return pltpu.make_async_remote_copy(
            src_ref=src, dst_ref=dst, send_sem=send, recv_sem=recv,
            device_id=where, device_id_type=MESH)

    def apiece(u, m):
        return abuf.at[u, group(m)]

    def group(m):
        return pl.ds(pl.multiple_of(m * RB, RB), RB)

    def load(w, act_local, act_remote):
        u = 2 * w + l
        mine = a_hbm.at[pl.ds(pl.multiple_of(l * half + w * RB, RB), RB)]
        other = a_hbm.at[pl.ds(pl.multiple_of((1 - l) * half + w * RB, RB), RB)]

        def place(spot):
            if act_local is not None:
                act_local(pltpu.make_async_copy(mine, spot, la.at[w]))
            if act_remote is not None:
                act_remote(remote(other, spot, ls, lr.at[w], layer=1 - l))

        @pl.when(home)
        def _():
            place(apiece(u, i))

        @pl.when(jnp.logical_not(home))
        def _():
            place(tbuf.at[u, z])

    def loaded(u):
        w = lax.div(u, 2)
        h = lax.rem(u, 2)

        @pl.when(h == l)
        def _():
            pltpu.make_async_copy(tbuf.at[u, z], tbuf.at[u, z], la.at[w]).wait()

        @pl.when(h != l)
        def _():
            remote(tbuf.at[u, z], tbuf.at[u, z], ls, lr.at[w], layer=1 - l).wait_recv()

    def part(p):
        return pl.ds(p * TN if isinstance(p, int) else pl.multiple_of(p * TN, TN), TN)

    def b_load(p):
        return pltpu.make_async_copy(b_hbm.at[:, part(p)], bbuf.at[l, :, part(p)], lb.at[p])

    def b_swap(p):
        return remote(b_hbm.at[:, part(p)], bbuf.at[l, :, part(p)], bs, br.at[p], layer=1 - l)

    def cross(u, k, act):
        @pl.when(k == dn)
        def _():
            act(remote(tbuf.at[u, k], rbuf.at[u], tx.at[k], rr.at[u], row=xn))

        @pl.when(k != dn)
        def _():
            act(remote(tbuf.at[u, k], apiece(u, i), tx.at[k], ar.at[u, i], row=k))

    def relay(u):
        return remote(rbuf.at[u], apiece(u, xn), rs, ar.at[u, xn], row=yn)

    relaying = (z == yn) | ((xn == last) & (yn < z)) | ((xn == 0) & (yn > z))

    def onward(u, k, act):
        for side, step in ((last, 1), (0, -1)):
            @pl.when((i == side) & (z != side))
            def _():
                act(remote(tbuf.at[u, k], tbuf.at[u, k], tz.at[k], tr.at[u, jnp.abs(k - z)], col=z + step))

    def passing(act):
        for d in range(1, R):
            for side, step in ((last, -1), (0, 1)):
                k = z + step * d

                @pl.when((i == side) & (k >= 0) & (k < R))
                def _():
                    act(k, d)

    def forward(u, m, act):
        @pl.when((m < last) & (i <= z) & (z < last))
        def _():
            act(remote(apiece(u, m), apiece(u, m), us.at[m], ar.at[u, m], col=z + 1))

        @pl.when((m > 0) & (i >= z) & (z > 0))
        def _():
            act(remote(apiece(u, m), apiece(u, m), ws.at[m], ar.at[u, m], col=z - 1))

    def arrived(u, m):
        return remote(apiece(u, m), apiece(u, m), us.at[m], ar.at[u, m], row=xn)

    def x_first(r):
        return (r == 1) | (r == 2) | ((r == 0) & (z == 2)) | ((r == 3) & (z == 1))

    here_x = x_first(i)
    side_x = x_first(xn)
    side_y = jnp.logical_not(x_first(yn))

    def far(v, act):
        @pl.when(here_x)
        def _():
            act(remote(cbuf.at[v, group(dn)], dxin.at[v], cd, dxr.at[v], row=xn))

        @pl.when(jnp.logical_not(here_x))
        def _():
            act(remote(cbuf.at[v, group(dn)], dyin.at[v], cd, dyr.at[v], row=yn))

    def to_x(v):
        return remote(cbuf.at[v, group(xn)], sums.at[v, 0], cx, sr.at[v], row=xn)

    def to_y(v):
        return remote(cbuf.at[v, group(yn)], sums.at[v, 1], cy, sr.at[v], row=yn)

    def out(v):
        return pltpu.make_async_copy(
            obuf.at[v], o_hbm.at[group(lax.div(v, NP)), part(lax.rem(v, NP))], lo)

    @pl.loop(0, NU // 2)
    def _(w):
        load(w, lambda t: t.start(), None)

    barrier = pltpu.get_barrier_semaphore()
    for where in ({"layer": 1 - l}, {"row": xn}, {"row": yn}, {"row": dn}):
        pl.semaphore_signal(barrier, inc=1, device_id=where, device_id_type=MESH)

    @pl.when(z > 0)
    def _():
        pl.semaphore_signal(barrier, inc=1, device_id={"col": z - 1}, device_id_type=MESH)

    @pl.when(z < last)
    def _():
        pl.semaphore_signal(barrier, inc=1, device_id={"col": z + 1}, device_id_type=MESH)

    pl.semaphore_wait(barrier, 4 + (z > 0).astype(jnp.int32) + (z < last).astype(jnp.int32))

    @pl.loop(0, NU // 2)
    def _(w):
        load(w, None, lambda t: t.start())

    def launch(u):
        loaded(u)

        @pl.when(jnp.logical_not(home))
        def _():
            cross(u, z, lambda t: t.start())

    def leave(u):
        @pl.when(jnp.logical_not(home))
        def _():
            onward(u, z, lambda t: t.start())

    def pass_on(s):
        def act(k, d):
            u = s - HOP * d + RIDE

            @pl.when((u >= 0) & (u < NU))
            def _():
                remote(tbuf.at[u, k], tbuf.at[u, k], tz.at[k], tr.at[u, d - 1], row=xn).wait_recv()
                onward(u, k, lambda t: t.start())
                cross(u, k, lambda t: t.start())
        passing(act)

    def hand_on(u):
        @pl.when(relaying)
        def _():
            remote(rbuf.at[u], rbuf.at[u], rs, rr.at[u], row=xn).wait_recv()
            relay(u).start()

    def depart(u):
        @pl.when(jnp.logical_not(home))
        def _():
            arrived(u, i).wait_recv()

        forward(u, i, lambda t: t.start())

    def spread(u):
        for m in (xn, yn, dn):
            wanted = home | ((i < z) & (m < last)) | ((i > z) & (m > 0))

            @pl.when(wanted)
            def _():
                arrived(u, m).wait_recv()
                forward(u, m, lambda t: t.start())

    def multiply(v):
        g = lax.div(v, NP)
        p = lax.rem(v, NP)

        @pl.when(p == 0)
        def _():
            @pl.when(i < z)
            def _():
                for e in range(2):
                    arrived(2 * g + e, last).wait_recv()

            @pl.when(i > z)
            def _():
                for e in range(2):
                    arrived(2 * g + e, 0).wait_recv()

        dots(v, 0)

    def dots(v, e):
        g = lax.div(v, NP)
        width = TN // 2
        columns = pl.ds(pl.multiple_of(lax.rem(v, NP) * TN + e * width, width), width)
        cbuf[v, :, e * width:(e + 1) * width] = (
            jnp.dot(abuf[2 * g], bbuf[0, :, columns], preferred_element_type=jnp.float32)
            + jnp.dot(abuf[2 * g + 1], bbuf[1, :, columns], preferred_element_type=jnp.float32))

    def partials(v):
        dots(v, 1)
        far(v, lambda t: t.start())

        @pl.when(jnp.logical_not(side_y))
        def _():
            to_x(v).start()

        @pl.when(jnp.logical_not(side_x))
        def _():
            to_y(v).start()

    def settle_x(v):
        @pl.when(side_y)
        def _():
            remote(dyin.at[v], dyin.at[v], cd, dyr.at[v], row=yn).wait_recv()
            cbuf[v, group(xn)] = cbuf[v, group(xn)] + dyin[v]
            to_x(v).start()

    def settle_y(v):
        @pl.when(side_x)
        def _():
            remote(dxin.at[v], dxin.at[v], cd, dxr.at[v], row=xn).wait_recv()
            cbuf[v, group(yn)] = cbuf[v, group(yn)] + dxin[v]
            to_y(v).start()

    def finish(v):
        remote(sums.at[v], sums.at[v], cx, sr.at[v], row=xn).wait_recv()
        obuf[v] = (cbuf[v, group(i)] + sums[v, 0] + sums[v, 1]).astype(jnp.bfloat16)
        out(v).start()

    away = HOP * jnp.abs(z - i)
    ML = 1 + LAG
    RL = RELAY + jnp.where(z == yn, -AHEAD, HOP * jnp.abs(z - yn) - RIDE)
    SL = HOP * last + ML + 1 + SETTLE
    FL = SL + FINISH

    @pl.loop(-max(AHEAD, RIDE, DEPART), NU + FL)
    def _(s):
        def at(lag, total, act):
            c = s - lag

            @pl.when((c >= 0) & (c < total))
            def _():
                act(c)

        for p in range(NP):
            @pl.when(s == BSTEP)
            def _():
                b_load(p).start()
                b_swap(p).start()

        at(-AHEAD, NU, launch)
        at(-RIDE, NU, leave)
        at(away - DEPART, NU, depart)
        at(RL, NU, hand_on)
        pass_on(s)
        at(away + ML + 1, NV, partials)
        at(away, NU, spread)

        for p in range(NP):
            @pl.when(s == away + ML + p)
            def _():
                b_load(p).wait()
                b_swap(p).wait_recv()

        at(away + ML, NV, multiply)
        at(ML + 1 + SETTLE + jnp.maximum(away, HOP * jnp.abs(z - yn)), NV, settle_x)
        at(ML + 1 + SETTLE + jnp.maximum(away, HOP * jnp.abs(z - xn)), NV, settle_y)
        at(FL, NV, finish)

    def sent(ref, sem):
        remote(ref, ref, sem, rr.at[0], row=xn).wait_send()

    def sent_on(k):
        sent(tbuf.at[:, k], tx.at[k])

        @pl.when(((i == last) & (z != last)) | ((i == 0) & (z != 0)))
        def _():
            sent(tbuf.at[:, k], tz.at[k])

    @pl.when(jnp.logical_not(home))
    def _():
        sent_on(z)

    passing(lambda k, d: sent_on(k))

    for m in range(R):
        @pl.when((m < last) & (i <= z) & (z < last))
        def _():
            sent(tbuf.at[:, m], us.at[m])

        @pl.when((m > 0) & (i >= z) & (z > 0))
        def _():
            sent(tbuf.at[:, m], ws.at[m])

    @pl.when(relaying)
    def _():
        sent(rbuf, rs)

    sent(tbuf.at[pl.ds(0, NU // 2), 0], ls)
    sent(bbuf.at[l], bs)
    sent(dxin, cd)
    sent(dxin, cx)
    sent(dxin, cy)
    pltpu.make_async_copy(obuf, obuf, lo).wait()


def plain(left_matrix, right_matrix):
    left_rows = lax.all_gather(left_matrix, "col", axis=1, tiled=True)
    right_joined = lax.all_gather(right_matrix, "row", axis=0, tiled=True)
    summed = lax.psum_scatter(
        jnp.dot(left_rows, right_joined, preferred_element_type=jnp.float32),
        "layer",
        scatter_dimension=0,
        tiled=True,
    )
    return summed.astype(jnp.bfloat16)


def fused(R, left_matrix, right_matrix):
    rows, K = left_matrix.shape
    N = right_matrix.shape[1]
    half, RB, NP = rows // 2, PIECE_ROWS, PARTS
    NU, TN, GB = 2 * half // RB, N // NP, RB
    NV = NU // 2 * NP
    bf16, f32 = jnp.bfloat16, jnp.float32
    dma = pltpu.SemaphoreType.DMA
    return pl.pallas_call(
        functools.partial(kernel, R, NU, RB, TN),
        out_shape=jax.ShapeDtypeStruct((half, N), bf16),
        in_specs=[pl.BlockSpec(memory_space=pl.ANY)] * 2,
        out_specs=pl.BlockSpec(memory_space=pl.ANY),
        scratch_shapes=[
            pltpu.VMEM((NU, R * RB, K), bf16),
            pltpu.VMEM((NU, R, RB, K), bf16),
            pltpu.VMEM((NU, RB, K), bf16),
            pltpu.VMEM((2, K, N), bf16),
            pltpu.VMEM((NV, R * GB, TN), f32),
            pltpu.VMEM((NV, GB, TN), f32),
            pltpu.VMEM((NV, GB, TN), f32),
            pltpu.VMEM((NV, 2, GB, TN), f32),
            pltpu.VMEM((NV, GB, TN), bf16),
            dma((NU // 2,)), dma, dma((NU // 2,)),
            dma((NP,)), dma, dma((NP,)),
            dma((NU, R)), dma((R,)), dma((R,)),
            dma((NU, R - 1)), dma((R,)), dma((R,)),
            dma((NU,)), dma,
            dma, dma((NV,)), dma((NV,)),
            dma, dma, dma((NV,)),
            dma,
        ],
        compiler_params=pltpu.CompilerParams(
            collective_id=0, has_side_effects=True, vmem_limit_bytes=67043328),
    )(left_matrix, right_matrix)


def solution(mesh):
    shape = mesh.shape
    fits = shape["layer"] == 2 and shape["row"] == shape["col"] == 4
    local = functools.partial(fused, shape["row"]) if fits else plain
    in_specs = (P("row", ("layer", "col")), P(("layer", "row"), "col"))
    out_specs = P(("row", "layer"), "col")
    return jax.shard_map(local, mesh=mesh, in_specs=in_specs, out_specs=out_specs, check_vma=False)
```
